32 devices in a mesh: ep: 8 (over y, x, core), fs: 4 (over z).
Axes of the slice: x: 2, y: 2, z: 4, core: 2. Of those that a mesh axis runs over, the one named last changes fastest.
Arguments:
- tokens: bfloat16 [6144, 2048], P(('ep', 'fs')), may hold values from -6 to 6
- attn_gain: bfloat16 [2048], P('fs'), may hold values from 0.5 to 1.5
- w_query: bfloat16 [2048, 2048], P('fs'), may hold values from -0.125 to 0.125
- w_key: bfloat16 [2048, 2048], P('fs'), may hold values from -0.125 to 0.125
- w_value: bfloat16 [2048, 2048], P('fs'), may hold values from -0.125 to 0.125
- query_gain: bfloat16 [128], P('fs'), may hold values from 0.5 to 1.5
- key_gain: bfloat16 [128], P('fs'), may hold values from 0.5 to 1.5
- w_output: bfloat16 [2048, 2048], P('fs'), may hold values from -2 to 2
- ffn_gain: bfloat16 [2048], P('fs'), may hold values from 0.5 to 1.5
- w_router: bfloat16 [2048, 32], P('fs'), may hold values from -0.0625 to 0.0625
- w_gate: bfloat16 [32, 2048, 1024], P('ep', 'fs'), may hold values from -0.125 to 0.125
- w_up: bfloat16 [32, 2048, 1024], P('ep', 'fs'), may hold values from -0.125 to 0.125
- w_down: bfloat16 [32, 1024, 2048], P('ep', 'fs'), may hold values from -0.5 to 0.5
- seq_lengths: int32 [8, 3], P('ep'), may hold values from 48 to 576, as said below
- span_places: int32 [8, 24], P('ep'), may hold values from 0 to 23, each once within a row
- routes: int32 [6144, 8], P(('ep', 'fs')), may hold values from 0 to 31, all different within a row; in each aligned block of 192 rows (0 to 191, 192 to 383, ...) at most 64 rows name the same one
- out_grad: bfloat16 [6144, 2048], P(('ep', 'fs')), may hold values from -6 to 6
Outputs:
- output: bfloat16 [6144, 2048], P(('ep', 'fs'))
- tokens_grad: bfloat16 [6144, 2048], P(('ep', 'fs'))
- attn_gain_grad: float32 [2048], P(('ep', 'fs'))
- w_query_grad: float32 [2048, 2048], P(('ep', 'fs'))
- w_key_grad: float32 [2048, 2048], P(('ep', 'fs'))
- w_value_grad: float32 [2048, 2048], P(('ep', 'fs'))
- query_gain_grad: float32 [128], P(('ep', 'fs'))
- key_gain_grad: float32 [128], P(('ep', 'fs'))
- w_output_grad: float32 [2048, 2048], P(('ep', 'fs'))
- ffn_gain_grad: float32 [2048], P(('ep', 'fs'))
- w_router_grad: float32 [2048, 32], P(('ep', 'fs'))
- w_gate_grad: float32 [32, 2048, 1024], P('ep', 'fs')
- w_up_grad: float32 [32, 2048, 1024], P('ep', 'fs')
- w_down_grad: float32 [32, 1024, 2048], P('ep', 'fs')
The draws below stay inside these ranges and needn't reach their ends.
Inputs may be any that keep to these rules, and one draw needn't show every extreme that they name: `seq_lengths`: in each group the 3 lengths sum to 768; the longest is exactly 576. `span_places`: each row is a permutation of the group's span places. `routes`: each row names 8 distinct experts; among the rows of one device no expert is named more than 64 times, and in some device some expert exactly 64 times.
All inputs are finite; a program needn't handle non-finite values.
Results may differ from the reference program's by a relative error of at most 0.025.
Values may be sent and summed in bfloat16 or wider, within the bound.
A program may use at most 384 MiB of HBM per device.

```python
import math
from functools import partial
import jax
import jax.numpy as jnp
import numpy as np
from jax import lax

D = 2048
HEADS = 16
HEAD_DIM = 128
FF = 1024
TOPK = 8
TOK_DEV = 192
SPAN = 32
SEQS = 3
EXPERTS = 32
GROUP = 768
MOST = 576
SPANS = 24
TOKENS = 6144
CAP = 64
N_EP = 8
N_FS = 4


def draw_seq_lengths(key, part):
    key_short, key_order = jax.random.split(jax.random.fold_in(key, 11))
    shorter = jax.random.randint(key_short, (N_EP,), GROUP // 16, GROUP // 4 - GROUP // 16 + 1).astype(jnp.int32)
    lengths_table = jnp.stack([jnp.full((N_EP,), MOST, jnp.int32), shorter, (GROUP // 4 - shorter).astype(jnp.int32)], axis=1)
    ranking = jax.random.randint(key_order, (N_EP, SEQS), 0, 1 << 20) * SEQS + jnp.arange(SEQS, dtype=jnp.int32)[None, :]
    arrangement = jnp.argsort(ranking, axis=1)
    return jnp.take_along_axis(lengths_table, arrangement, axis=1).astype(jnp.int32)


def steps_of(key, dims, cuts, least, high):
    def one(dim, shards_of):
        heights = jax.random.uniform(jax.random.fold_in(jax.random.fold_in(key, 6), dim), (shards_of,), jnp.float32, least / len(cuts), high / len(cuts))
        return jnp.repeat(jnp.exp(heights), dims[dim] // shards_of).reshape((-1,) + (1,) * (len(dims) - dim - 1))

    factor_of = one(*cuts[0])
    for cut in cuts[1:]:
        factor_of = factor_of * one(*cut)
    return factor_of


def assign_block(stream_key, own, number, rows, number_of, top, bound, skew):
    order = jax.random.permutation(stream_key, number_of)
    packed, common = portions_of(number_of, rows * top, bound, skew, True), portions_of(number_of, rows * top, bound, skew, False)
    places = jnp.arange(number_of)

    def named(sizes, turn):
        used = int((sizes > 0).sum())
        fixed = max(1, used // 4)
        passed = fixed + (places - fixed + turn * (used - fixed)) % max(1, number_of - fixed)
        return jnp.zeros((number_of,), jnp.int32).at[order[jnp.where(places < fixed, places, passed)]].set(jnp.asarray(sizes, jnp.int32))

    sizes = jnp.where(number % 4 == 0, named(packed, number // 4), named(common, number - number // 4 - 1))
    mixed = jax.random.permutation(jax.random.fold_in(own, 3), number_of)
    donor, sink = mixed[0:number_of // 2 * 2:2], mixed[1:number_of // 2 * 2:2]
    margin = jnp.minimum(sizes[donor] - 1, bound - sizes[sink]) // 2
    margin = jnp.where((donor == order[0]) | (sink == order[0]) | (sizes[sink] == 0), 0, jnp.maximum(margin, 0))
    passed = jax.random.randint(jax.random.fold_in(own, 4), (number_of // 2,), 0, 1 << 20) % (margin + 1)
    sizes = sizes.at[donor].add(-passed).at[sink].add(passed)
    members = jnp.searchsorted(jnp.cumsum(sizes), jnp.arange(rows * top), side="right").astype(jnp.int32)
    table = members.reshape(top, rows).T
    table = table[jax.random.permutation(jax.random.fold_in(own, 1), rows)]
    turn = jax.random.randint(jax.random.fold_in(own, 2), (rows, 1), 0, top)
    return jnp.take_along_axis(table, (jnp.arange(top)[None, :] + turn) % top, axis=1)


def portions_of(count, total, bound, lean, full):
    weights = [(1 << 20) // math.isqrt(grade ** lean) + 1 for grade in range(1, count + 1)]
    largest = bound if full else min(bound, max(-(-total // count), total * weights[0] // sum(weights)))
    least = 1 if total - largest >= count - 1 else 0
    counts, spare = [largest] + [least] * (count - 1), total - largest - least * (count - 1)
    while spare > 0:
        free = [i for i in range(1, count) if counts[i] < largest] or [i for i in range(1, count) if counts[i] < bound]
        whole, budget = sum([weights[i] for i in free]), spare
        for i in free:
            addition = min(bound - counts[i], max(1, budget * weights[i] // whole), spare)
            counts[i] = counts[i] + addition
            spare = spare - addition
    return np.array(counts)


def normal_values(stream_key, shape, width, limit, cuts=(), kind=jnp.bfloat16):
    loudness = steps_of(stream_key, shape, cuts, -0.22, 0.18) if cuts else 1.0
    drawn = jax.random.normal(stream_key, shape, jnp.float32) * width * loudness
    return jnp.minimum(jnp.maximum(drawn, -limit), limit).astype(kind)


def setup_inputs(seed: int = 0) -> dict:
    seeds = jax.random.split(jax.random.key(seed), 18)
    tokens = normal_values(seeds[0], (TOKENS, D), 1.0, 6.0, ((0, 32),))
    attn_gain = jnp.clip(1.0 + 0.1 * jax.random.normal(seeds[1], (D,), jnp.float32), 0.5, 1.5).astype(jnp.bfloat16)
    w_query = normal_values(seeds[2], (D, D), D ** -0.5, 0.125, ((0, 4),))
    w_key = normal_values(seeds[3], (D, D), D ** -0.5, 0.125, ((0, 4),))
    w_value = normal_values(seeds[4], (D, D), D ** -0.5, 0.125, ((0, 4),))
    query_gain = jnp.clip(1.0 + 0.1 * jax.random.normal(seeds[5], (HEAD_DIM,), jnp.float32), 0.5, 1.5).astype(jnp.bfloat16)
    key_gain = jnp.clip(1.0 + 0.1 * jax.random.normal(seeds[6], (HEAD_DIM,), jnp.float32), 0.5, 1.5).astype(jnp.bfloat16)
    w_output = normal_values(seeds[7], (D, D), (max(8, D // 256)) ** -0.5, 2.0, ((0, 4),))
    ffn_gain = jnp.clip(1.0 + 0.1 * jax.random.normal(seeds[8], (D,), jnp.float32), 0.5, 1.5).astype(jnp.bfloat16)
    w_router = normal_values(seeds[9], (D, EXPERTS), (4 * D) ** -0.5, 0.0625, ((0, 4),))
    w_gate = normal_values(seeds[10], (EXPERTS, D, FF), D ** -0.5, 0.125, ((0, 8), (1, 4)))
    w_up = normal_values(seeds[11], (EXPERTS, D, FF), D ** -0.5, 0.125, ((0, 8), (1, 4)))
    w_down = normal_values(seeds[12], (EXPERTS, FF, D), (FF // 8) ** -0.5, 0.5, ((0, 8), (1, 4)))
    seq_lengths = draw_seq_lengths(jax.random.fold_in(seeds[17], 71), 0)
    span_places = jax.vmap(lambda own: jax.random.permutation(own, SPANS))(jax.random.split(seeds[14], N_EP)).reshape((N_EP, SPANS)).astype(jnp.int32)
    routes_keys = jax.random.split(jax.random.fold_in(seeds[15], 1), TOKENS // TOK_DEV)
    routes_turns = jax.random.permutation(jax.random.fold_in(seeds[15], 3), TOKENS // TOK_DEV)
    routes = jax.vmap(lambda own, number: assign_block(jax.random.fold_in(seeds[15], 2), own, number, TOK_DEV, EXPERTS, TOPK, CAP, 2))(routes_keys, routes_turns).reshape((TOKENS, TOPK))
    out_grad = normal_values(seeds[16], (TOKENS, D), 1.0, 6.0, ((0, 32),))
    return {"tokens": tokens, "attn_gain": attn_gain, "w_query": w_query, "w_key": w_key, "w_value": w_value, "query_gain": query_gain, "key_gain": key_gain, "w_output": w_output, "ffn_gain": ffn_gain, "w_router": w_router, "w_gate": w_gate, "w_up": w_up, "w_down": w_down, "seq_lengths": seq_lengths, "span_places": span_places, "routes": routes, "out_grad": out_grad}


@jax.custom_vjp
def low(v):
    return lax.optimization_barrier(v.astype(jnp.bfloat16)).astype(jnp.float32)

@jax.custom_vjp
def low_back(v):
    return v

def low_keep(v):
    return (low(v), None)

def low_pass(kept, grad):
    return (grad,)

def back_keep(v):
    return (v, None)

def back_low(kept, grad):
    return (low(grad),)
low.defvjp(low_keep, low_pass)
low_back.defvjp(back_keep, back_low)
epsilon = 1e-06
rope_base = 10000.0
highest = lax.Precision.HIGHEST

def rms_scale(values):
    return lax.rsqrt(lax.optimization_barrier(jnp.mean(values * values, axis=-1, keepdims=True)) + epsilon)

def rope_tables(position, half_dim, head_dim):
    inverse = jnp.exp(jnp.arange(half_dim).astype(jnp.float32) * (-2.0 * math.log(rope_base) / head_dim))
    angles = position.astype(jnp.float32)[:, None] * inverse[None, :]
    return (jnp.cos(angles), jnp.sin(angles))

def rotate(values, cosines, sines):
    half_dim = values.shape[-1] // 2
    former = values[..., :half_dim]
    latter = values[..., half_dim:]
    return jnp.concatenate([former * cosines - latter * sines, latter * cosines + former * sines], axis=-1)

def group_layout(lengths_row, places_row, group_rows, span_rows):
    arrival = jnp.arange(group_rows, dtype=jnp.int32)
    span_hit = (arrival // span_rows)[:, None] == jnp.arange(places_row.shape[0], dtype=jnp.int32)[None, :]
    places = (lax.optimization_barrier(jnp.sum(jnp.where(span_hit, places_row[None, :], 0), axis=1)) * span_rows + arrival % span_rows).astype(jnp.int32)
    seq_ends = jnp.cumsum(lengths_row).astype(jnp.int32)
    segment = lax.optimization_barrier(jnp.sum((places[:, None] >= seq_ends[None, :]).astype(jnp.int32), axis=1)).astype(jnp.int32)
    seq_starts = (seq_ends - lengths_row).astype(jnp.int32)
    picked = segment[:, None] == jnp.arange(lengths_row.shape[0], dtype=jnp.int32)[None, :]
    position = (places - lax.optimization_barrier(jnp.sum(jnp.where(picked, seq_starts[None, :], 0), axis=1))).astype(jnp.int32)
    return (segment, position)

def slot_tables(routes):
    devices = N_EP * N_FS
    pair_rows = TOK_DEV * TOPK
    blocks = routes.reshape(devices, pair_rows).astype(jnp.int32)
    matches = (blocks[:, :, None] == jnp.arange(EXPERTS, dtype=jnp.int32)[None, None, :]).astype(jnp.int32)
    slot_rank = lax.optimization_barrier(jnp.sum((jnp.cumsum(matches, axis=1) - 1) * matches, axis=2)).astype(jnp.int32)
    block_ids = jnp.arange(devices, dtype=jnp.int32)[:, None]
    local_ids = jnp.arange(pair_rows, dtype=jnp.int32)[None, :]
    columns = (block_ids * CAP + slot_rank).astype(jnp.int32)
    token_ids = jnp.broadcast_to(block_ids * TOK_DEV + local_ids // TOPK, blocks.shape).astype(jnp.int32)
    pair_ids = jnp.broadcast_to(block_ids * pair_rows + local_ids, blocks.shape).astype(jnp.int32)
    token_table = jnp.full((EXPERTS, devices * CAP), TOKENS, jnp.int32).at[blocks, columns].set(token_ids)
    pair_table = jnp.full((EXPERTS, devices * CAP), TOKENS * TOPK, jnp.int32).at[blocks, columns].set(pair_ids)
    return (token_table, pair_table)

def reference(tokens, attn_gain, w_query, w_key, w_value, query_gain, key_gain, w_output, ffn_gain, w_router, w_gate, w_up, w_down, seq_lengths, span_places, routes, out_grad):
    layout_fn = partial(group_layout, group_rows=GROUP, span_rows=SPAN)
    segment, position = jax.vmap(layout_fn)(seq_lengths, span_places)
    cosines, sines = rope_tables(position.reshape(TOKENS), HEAD_DIM // 2, HEAD_DIM)
    cosines = cosines[:, None, :]
    sines = sines[:, None, :]
    token_table, pair_table = slot_tables(routes)
    factor = 1.0 / math.sqrt(HEAD_DIM)
    floats = tuple((argument.astype(jnp.float32) for argument in (tokens, attn_gain, w_query, w_key, w_value, query_gain, key_gain, w_output, ffn_gain, w_router, w_gate, w_up, w_down)))

    def group_attention(block):
        queries, key_rows, value_rows, segment_row = block
        logits = jnp.einsum('ihd,jhd->hij', queries, key_rows, precision=highest) * factor
        allowed = (segment_row[:, None] == segment_row[None, :])[None]
        logits = low_back(jnp.where(allowed, logits, -1000000000.0))
        weights = low(jax.nn.softmax(logits, axis=-1))
        return jnp.einsum('hij,jhd->ihd', weights, value_rows, precision=highest)

    def forward(hidden_in, gain_one, query_w, key_w, value_w, gain_query, gain_key, output_w, gain_two, router_w, gate_w, up_w, down_w):
        normed_one = low(hidden_in * rms_scale(hidden_in) * gain_one)
        query_pre = low_back(jnp.dot(normed_one, query_w, precision=highest)).reshape(TOKENS, HEADS, HEAD_DIM)
        key_pre = low_back(jnp.dot(normed_one, key_w, precision=highest)).reshape(TOKENS, HEADS, HEAD_DIM)
        value_low = low(low_back(jnp.dot(normed_one, value_w, precision=highest))).reshape(TOKENS, HEADS, HEAD_DIM)
        query_rot = low(low_back(rotate(query_pre * rms_scale(query_pre) * gain_query, cosines, sines)))
        key_rot = low(low_back(rotate(key_pre * rms_scale(key_pre) * gain_key, cosines, sines)))
        attended = lax.map(jax.checkpoint(group_attention), (query_rot.reshape(N_EP, GROUP, HEADS, HEAD_DIM), key_rot.reshape(N_EP, GROUP, HEADS, HEAD_DIM), value_low.reshape(N_EP, GROUP, HEADS, HEAD_DIM), segment))
        attended_low = low(low_back(attended.reshape(TOKENS, D)))
        hidden_mid = hidden_in + low_back(jnp.dot(attended_low, output_w, precision=highest))
        normed_two = low(hidden_mid * rms_scale(hidden_mid) * gain_two)
        logits = low_back(jnp.dot(normed_two, router_w, precision=highest))
        chosen = jnp.take_along_axis(logits, routes, axis=1)
        gates = jax.nn.softmax(chosen, axis=-1)
        padded_rows = jnp.concatenate([normed_two, jnp.zeros((1, D), jnp.float32)], axis=0)
        padded_gates = jnp.concatenate([gates.reshape(TOKENS * TOPK), jnp.zeros((1,), jnp.float32)])

        def expert_rows(block):
            gate_matrix, up_matrix, down_matrix, token_row = block
            inputs = low_back(padded_rows[token_row])
            gate_pre = low_back(jnp.dot(inputs, gate_matrix, precision=highest))
            up_pre = low_back(jnp.dot(inputs, up_matrix, precision=highest))
            activated = low(jax.nn.silu(gate_pre) * up_pre)
            return low(low_back(jnp.dot(activated, down_matrix, precision=highest)))
        results = lax.map(jax.checkpoint(expert_rows), (gate_w, up_w, down_w, token_table))
        weighted = results * padded_gates[pair_table][:, :, None]
        mixed = jnp.zeros((TOKENS + 1, D), jnp.float32).at[token_table].add(weighted)[:TOKENS]
        return hidden_mid + mixed
    result, pullback = jax.vjp(forward, *floats)
    grads = pullback(out_grad.astype(jnp.float32))
    return (result.astype(jnp.bfloat16), grads[0].astype(jnp.bfloat16), grads[1], grads[2], grads[3], grads[4], grads[5], grads[6], grads[7], grads[8], grads[9], grads[10], grads[11], grads[12])
```

```python
import math

import jax
import jax.numpy as jnp
from jax import lax
from jax.experimental import pallas as pl
from jax.experimental.pallas import tpu as pltpu
from jax.sharding import PartitionSpec as P

epsilon = 1e-06
rope_base = 10000.0
masked_score = -1000000000.0
low_type = jnp.bfloat16
VMEM_LIMIT = 66_000_000


def rms_scale(values):
    return lax.rsqrt(jnp.mean(values * values, axis=-1, keepdims=True) + epsilon)


def mm(a, b, dims):
    return lax.dot_general(a, b, (dims, ((), ())), preferred_element_type=jnp.float32)


NN = ((1,), (0,))
NT = ((1,), (1,))
TN = ((0,), (0,))


def norm_back(values, scale, gain, upstream):
    weighted = upstream * gain
    inner_mean = jnp.mean(weighted * values, axis=-1, keepdims=True)
    return (
        scale * weighted - values * (scale * scale * scale) * inner_mean,
        upstream * values * scale,
    )


def group_layout(lengths_row, places_row, group_rows, span_rows):
    arrival = jnp.arange(group_rows, dtype=jnp.int32)
    span_hit = (arrival // span_rows)[:, None] == jnp.arange(places_row.shape[0], dtype=jnp.int32)[
        None, :
    ]
    places = (
        jnp.sum(jnp.where(span_hit, places_row[None, :], 0), axis=1) * span_rows
        + arrival % span_rows
    )
    seq_ends = jnp.cumsum(lengths_row)
    segment = jnp.sum((places[:, None] >= seq_ends[None, :]).astype(jnp.int32), axis=1)
    seq_starts = seq_ends - lengths_row
    picked = segment[:, None] == jnp.arange(lengths_row.shape[0], dtype=jnp.int32)[None, :]
    position = places - jnp.sum(jnp.where(picked, seq_starts[None, :], 0), axis=1)
    return (segment, position)


def rotated(pre, gain, cos2, sin2):
    scale = rms_scale(pre)
    normed = pre * scale * gain
    half = pre.shape[1] // 2
    return scale, normed * cos2 + pltpu.roll(normed, half, 1) * sin2


def attn_forward_kernel(
    q_ref, k_ref, v_ref, gq_ref, gk_ref, cos_ref, sin_ref, segc_ref, segr_ref, o_ref, q_scr, *, block
):
    rows = q_ref.shape[0]
    factor = 1.0 / math.sqrt(q_ref.shape[1])
    cos2 = cos_ref[...]
    sin2 = sin_ref[...]
    q_scr[...] = rotated(q_ref[...], gq_ref[...], cos2, sin2)[1].astype(low_type)
    key = rotated(k_ref[...], gk_ref[...], cos2, sin2)[1].astype(low_type)
    value = v_ref[...].astype(low_type)

    def step(i, carry):
        at = pl.ds(pl.multiple_of(i * block, block), block)
        raw = mm(q_scr[at, :], key, NT) * factor
        raw = jnp.where(segc_ref[at, :] == segr_ref[...], raw, masked_score)
        peak = jnp.max(raw, axis=1, keepdims=True)
        powers = jnp.exp(raw - peak)
        weights = powers / jnp.sum(powers, axis=1, keepdims=True)
        o_ref[at, :] = mm(weights.astype(low_type), value, NN).astype(low_type)
        return carry

    lax.fori_loop(0, rows // block, step, 0)


def attn_backward_kernel(
    q_ref,
    k_ref,
    v_ref,
    da_ref,
    gq_ref,
    gk_ref,
    cos_ref,
    sin_ref,
    segc_ref,
    segr_ref,
    dq_ref,
    dk_ref,
    dv_ref,
    dgq_ref,
    dgk_ref,
    q_scr,
    dq_scr,
    dk_scr,
    dv_scr,
    *,
    block,
):
    rows, head_dim = q_ref.shape
    factor = 1.0 / math.sqrt(head_dim)
    cos2 = cos_ref[...]
    sin2 = sin_ref[...]
    q_scale, q_rot = rotated(q_ref[...], gq_ref[...], cos2, sin2)
    q_scr[...] = q_rot.astype(low_type)
    k_scale, k_rot = rotated(k_ref[...], gk_ref[...], cos2, sin2)
    key = k_rot.astype(low_type)
    value = v_ref[...].astype(low_type)
    dk_scr[...] = jnp.zeros_like(dk_scr)
    dv_scr[...] = jnp.zeros_like(dv_scr)

    def step(i, carry):
        at = pl.ds(pl.multiple_of(i * block, block), block)
        query = q_scr[at, :]
        grads = da_ref[at, :]
        raw = mm(query, key, NT) * factor
        raw = jnp.where(segc_ref[at, :] == segr_ref[...], raw, masked_score)
        peak = jnp.max(raw, axis=1, keepdims=True)
        powers = jnp.exp(raw - peak)
        probs = powers / jnp.sum(powers, axis=1, keepdims=True)
        grad_probs = mm(grads, value, NT)
        delta = jnp.sum(probs * grad_probs, axis=1, keepdims=True)
        grad_scores = (probs * (grad_probs - delta)).astype(low_type)
        dq_scr[at, :] = mm(grad_scores, key, NN) * factor
        dk_scr[...] += mm(grad_scores, query, TN)
        dv_scr[...] += mm(probs.astype(low_type), grads, TN)
        return carry

    lax.fori_loop(0, rows // block, step, 0)
    half = head_dim // 2

    def finish(pre, scale, gain, upstream, out_ref, gain_out_ref):
        upstream = upstream.astype(low_type).astype(jnp.float32)
        back = upstream * cos2 - pltpu.roll(upstream, half, 1) * sin2
        grad_pre, gain_terms = norm_back(pre, scale, gain, back)
        out_ref[...] = grad_pre.astype(low_type)
        gain_out_ref[0] = jnp.sum(gain_terms, axis=0, keepdims=True)

    finish(q_ref[...], q_scale, gq_ref[...], dq_scr[...], dq_ref, dgq_ref)
    finish(k_ref[...], k_scale, gk_ref[...], dk_scr[...] * factor, dk_ref, dgk_ref)
    dv_ref[...] = dv_scr[...].astype(low_type)


def attention_forward(qkv, gain_q, gain_k, cos2, sin2, segment, head_dim):
    rows, width3 = qkv.shape
    heads = width3 // (3 * head_dim)
    block = 256
    col = lambda part: pl.BlockSpec((rows, head_dim), lambda h: (0, part * heads + h))
    full = lambda shape: pl.BlockSpec(shape, lambda h: (0, 0))
    return pl.pallas_call(
        lambda *refs: attn_forward_kernel(*refs, block=block),
        grid=(heads,),
        in_specs=[
            col(0),
            col(1),
            col(2),
            full((1, head_dim)),
            full((1, head_dim)),
            full((rows, head_dim)),
            full((rows, head_dim)),
            full((rows, 1)),
            full((1, rows)),
        ],
        out_specs=pl.BlockSpec((rows, head_dim), lambda h: (0, h)),
        out_shape=jax.ShapeDtypeStruct((rows, heads * head_dim), low_type),
        scratch_shapes=[pltpu.VMEM((rows, head_dim), low_type)],
        compiler_params=pltpu.CompilerParams(vmem_limit_bytes=VMEM_LIMIT // 2),
        cost_estimate=pl.CostEstimate(
            flops=heads * rows * rows * head_dim * 4,
            bytes_accessed=rows * width3 * 4,
            transcendentals=heads * rows * rows,
        ),
        name="attn_forward",
    )(qkv, qkv, qkv, gain_q, gain_k, cos2, sin2, segment[:, None], segment[None, :])


def attention_backward(qkv, grad_attended, gain_q, gain_k, cos2, sin2, segment, head_dim):
    rows, width3 = qkv.shape
    heads = width3 // (3 * head_dim)
    block = 256
    col = lambda part: pl.BlockSpec((rows, head_dim), lambda h: (0, part * heads + h))
    full = lambda shape: pl.BlockSpec(shape, lambda h: (0, 0))
    wide = jax.ShapeDtypeStruct((rows, heads * head_dim), low_type)
    gain = jax.ShapeDtypeStruct((heads, 1, head_dim), jnp.float32)
    gain_spec = pl.BlockSpec((1, 1, head_dim), lambda h: (h, 0, 0))
    return pl.pallas_call(
        lambda *refs: attn_backward_kernel(*refs, block=block),
        grid=(heads,),
        in_specs=[
            col(0),
            col(1),
            col(2),
            col(0),
            full((1, head_dim)),
            full((1, head_dim)),
            full((rows, head_dim)),
            full((rows, head_dim)),
            full((rows, 1)),
            full((1, rows)),
        ],
        out_specs=[col(0), col(0), col(0), gain_spec, gain_spec],
        out_shape=[wide, wide, wide, gain, gain],
        scratch_shapes=[
            pltpu.VMEM((rows, head_dim), low_type),
            pltpu.VMEM((rows, head_dim), jnp.float32),
            pltpu.VMEM((rows, head_dim), jnp.float32),
            pltpu.VMEM((rows, head_dim), jnp.float32),
        ],
        compiler_params=pltpu.CompilerParams(vmem_limit_bytes=VMEM_LIMIT // 2),
        cost_estimate=pl.CostEstimate(
            flops=heads * rows * rows * head_dim * 10,
            bytes_accessed=rows * width3 * 6,
            transcendentals=heads * rows * rows,
        ),
        name="attn_backward",
    )(qkv, qkv, qkv, grad_attended, gain_q, gain_k, cos2, sin2, segment[:, None], segment[None, :])


def experts_kernel(place_ref, *refs, sources, cap, locals_, total, shards):
    x_ref, g_ref, rank_ref, router_ref = refs[:4]
    refs = refs[4:]
    gate_refs, up_refs, wd_ref = refs[:shards], refs[shards : 2 * shards], refs[2 * shards]
    refs = refs[2 * shards + 1 :]
    out_hbm, dx_hbm, dwd_hbm = refs[:3]
    dwg_hbm, dwu_hbm = refs[3 : 3 + shards], refs[3 + shards : 3 + 2 * shards]
    refs = refs[3 + 2 * shards :]
    x_slots, g_slots, gates_col, acc_g, acc_u, acc_d, out_stage, dx_stage = refs[:8]
    out_sem, dx_sem, acc_sem, grad_sem = refs[8:]
    b = pl.program_id(0)
    e = pl.program_id(1)
    blocks = pl.num_programs(0)
    rows = x_ref.shape[0] // sources
    width = x_ref.shape[1]
    chunk = width // shards
    slots = sources * cap
    me = place_ref[1]

    def one_hot(s):
        slot = lax.broadcasted_iota(jnp.int32, (cap, rows), 0)
        return [slot == rank_ref[s, j : j + 1, :] for j in range(locals_)]

    @pl.when(e == 0)
    def _():
        for s in range(sources):
            at = pl.ds(s * rows, rows)
            logits = mm(router_ref[...], x_ref[at, :], NT)
            live = rank_ref[s] >= 0
            kept = jnp.where(live, logits, -1e30)
            powers = jnp.where(live, jnp.exp(kept - jnp.max(kept, axis=0, keepdims=True)), 0.0)
            gates = powers / jnp.sum(powers, axis=0, keepdims=True)
            hits = one_hot(s)
            for j in range(locals_):
                picked = jnp.sum(
                    jnp.where(hits[j], gates[j : j + 1, :], 0.0), axis=1, keepdims=True
                )
                gates_col[j, s * cap : (s + 1) * cap, :] = jnp.broadcast_to(
                    picked, (cap, gates_col.shape[2])
                )
            select = jnp.concatenate([h.astype(jnp.float32) for h in hits], axis=0).astype(low_type)
            for c in range(0, width, chunk):
                picked_x = mm(select, x_ref[at, c : c + chunk], NN).astype(low_type)
                picked_g = mm(select, g_ref[at, c : c + chunk], NN).astype(low_type)
                for j in range(locals_):
                    x_slots[j, s * cap : (s + 1) * cap, c : c + chunk] = picked_x[
                        j * cap : (j + 1) * cap
                    ]
                    g_slots[j, s * cap : (s + 1) * cap, c : c + chunk] = picked_g[
                        j * cap : (j + 1) * cap
                    ]

    @pl.when(b == 0)
    def _():
        acc_g[e] = jnp.zeros(acc_g.shape[1:], jnp.float32)
        acc_u[e] = jnp.zeros(acc_u.shape[1:], jnp.float32)
        acc_d[e] = jnp.zeros(acc_d.shape[1:], jnp.float32)

    hidden = wd_ref.shape[1]
    gate = gates_col[e][:, :1]
    gs = g_slots[e, :slots, :width]
    gate_pre = jnp.zeros((slots, hidden), jnp.float32)
    up_pre = jnp.zeros((slots, hidden), jnp.float32)
    columns = [
        pl.ds(pl.multiple_of(lax.rem(me + shards - k, shards) * chunk, chunk), chunk)
        for k in range(shards)
    ]
    for k in range(shards):
        xs = x_slots[e, :slots, columns[k]]
        gate_pre += mm(xs, gate_refs[k][0], NN)
        up_pre += mm(xs, up_refs[k][0], NN)
    back = mm(gs, wd_ref[0], NT)
    sigmoid = jax.nn.sigmoid(gate_pre)
    silu = gate_pre * sigmoid
    activated = silu * up_pre
    grad_gate_dot = jnp.sum(
        activated.astype(low_type).astype(jnp.float32) * back, axis=1, keepdims=True
    )
    grad_act = back * gate
    grad_up = (grad_act * silu).astype(low_type)
    grad_gate = (grad_act * up_pre * sigmoid * (1.0 + gate_pre * (1.0 - sigmoid))).astype(low_type)
    act_gated = (activated * gate).astype(low_type)
    for c in range(0, width, chunk):
        cols = pl.ds(c, chunk)
        acc_g[e, :, cols] += mm(grad_gate, x_slots[e, :slots, cols], TN)
        acc_u[e, :, cols] += mm(grad_up, x_slots[e, :slots, cols], TN)
        acc_d[e, :, cols] += mm(act_gated, g_slots[e, :slots, cols], TN)
    for c in range(0, width, chunk):
        cols = pl.ds(c, chunk)
        x_slots[e, :slots, cols] = mm(act_gated, wd_ref[0, :, cols], NN).astype(low_type)
    for k in range(shards):
        g_slots[e, :slots, columns[k]] = (
            mm(grad_gate, gate_refs[k][0], NT) + mm(grad_up, up_refs[k][0], NT)
        ).astype(low_type)
    lanes = g_slots.shape[2] - width
    lane = lax.broadcasted_iota(jnp.int32, (slots, lanes), 1)
    high = grad_gate_dot.astype(low_type).astype(jnp.float32)
    mine = place_ref[0] + e
    g_slots[e, :slots, width:] = jnp.where(
        lane == mine, high, jnp.where(lane == mine + total, grad_gate_dot - high, 0.0)
    ).astype(low_type)

    @pl.when(e == pl.num_programs(1) - 1)
    def _():
        pending = [None, None]
        for s in range(sources):
            slot = s % 2
            if pending[slot] is not None:
                for copy in pending[slot]:
                    copy.wait()
            hits = one_hot(s)
            select = jnp.concatenate([h.astype(jnp.float32) for h in hits], axis=0).astype(low_type)
            part = slice(s * cap, (s + 1) * cap)
            for c in range(0, width, chunk):
                cols = slice(c, c + chunk)
                ys = jnp.concatenate([x_slots[j, part, cols] for j in range(locals_)], axis=0)
                out_stage[slot, :, cols] = mm(select, ys, TN).astype(low_type)
                ds_ = jnp.concatenate([g_slots[j, part, cols] for j in range(locals_)], axis=0)
                dx_stage[slot, :, cols] = mm(select, ds_, TN).astype(low_type)
            tail = jnp.concatenate([g_slots[j, part, width:] for j in range(locals_)], axis=0)
            dx_stage[slot, :, width:] = mm(select, tail, TN).astype(low_type)
            at = pl.ds((b * sources + s) * rows, rows)
            copies = (
                pltpu.make_async_copy(out_stage.at[slot], out_hbm.at[at], out_sem.at[slot]),
                pltpu.make_async_copy(dx_stage.at[slot], dx_hbm.at[at], dx_sem.at[slot]),
            )
            for copy in copies:
                copy.start()
            pending[slot] = copies
        for copies in pending:
            if copies is not None:
                for copy in copies:
                    copy.wait()

    @pl.when((b == blocks - 1) & (e == locals_ - 1))
    def _():
        copies = [pltpu.make_async_copy(acc_d, dwd_hbm, acc_sem)]
        copies[0].start()
        for j in range(locals_):
            x_slots[j, :hidden, :] = acc_g[j].astype(low_type)
            g_slots[j, :hidden, :width] = acc_u[j].astype(low_type)
            for k in range(shards):
                cols = pl.ds(pl.multiple_of(lax.rem(me + k, shards) * chunk, chunk), chunk)
                for which, (held, target) in enumerate(((x_slots, dwg_hbm), (g_slots, dwu_hbm))):
                    copy = pltpu.make_async_copy(
                        held.at[j, pl.ds(0, hidden), cols],
                        target[k].at[j],
                        grad_sem.at[which, j, k],
                    )
                    copy.start()
                    copies.append(copy)
        for copy in copies:
            copy.wait()


def run_experts(place, x_all, g_all, rank, router_rows, gate_parts, up_parts, w_down, cap):
    tokens_all, width = x_all.shape
    devices, total, rows = rank.shape
    shards = len(gate_parts)
    locals_, shard_rows, hidden = gate_parts[0].shape
    sources = 4
    blocks = devices // sources
    block_rows = sources * rows
    slots = sources * cap
    held_rows = max(slots, hidden)
    any_spec = pl.BlockSpec(memory_space=pl.ANY)
    weight_spec = pl.BlockSpec((1, shard_rows, hidden), lambda b, e, *_: (e, 0, 0))
    grid_spec = pltpu.PrefetchScalarGridSpec(
        num_scalar_prefetch=1,
        grid=(blocks, locals_),
        in_specs=[
            pl.BlockSpec((block_rows, width), lambda b, e, *_: (b, 0)),
            pl.BlockSpec((block_rows, width), lambda b, e, *_: (b, 0)),
            pl.BlockSpec((sources, total, rows), lambda b, e, *_: (b, 0, 0)),
            pl.BlockSpec((total, width), lambda b, e, *_: (0, 0)),
            *([weight_spec] * (2 * shards)),
            pl.BlockSpec((1, hidden, width), lambda b, e, *_: (e, 0, 0)),
        ],
        out_specs=[any_spec] * (3 + 2 * shards),
        scratch_shapes=[
            pltpu.VMEM((locals_, held_rows, width), low_type),
            pltpu.VMEM((locals_, held_rows, width + 128), low_type),
            pltpu.VMEM((locals_, slots, 128), jnp.float32),
            pltpu.VMEM((locals_, hidden, width), jnp.float32),
            pltpu.VMEM((locals_, hidden, width), jnp.float32),
            pltpu.VMEM((locals_, hidden, width), jnp.float32),
            pltpu.VMEM((2, rows, width), low_type),
            pltpu.VMEM((2, rows, width + 128), low_type),
            pltpu.SemaphoreType.DMA((2,)),
            pltpu.SemaphoreType.DMA((2,)),
            pltpu.SemaphoreType.DMA,
            pltpu.SemaphoreType.DMA((2, locals_, shards)),
        ],
    )
    piece = jax.ShapeDtypeStruct((locals_, hidden, shard_rows), low_type)
    got = pl.pallas_call(
        lambda *refs: experts_kernel(
            *refs, sources=sources, cap=cap, locals_=locals_, total=total, shards=shards
        ),
        grid_spec=grid_spec,
        out_shape=[
            jax.ShapeDtypeStruct((tokens_all, width), low_type),
            jax.ShapeDtypeStruct((tokens_all, width + 128), low_type),
            jax.ShapeDtypeStruct((locals_, hidden, width), jnp.float32),
            *([piece] * (2 * shards)),
        ],
        input_output_aliases={1: 0},
        compiler_params=pltpu.CompilerParams(vmem_limit_bytes=VMEM_LIMIT),
        cost_estimate=pl.CostEstimate(
            flops=18 * blocks * locals_ * slots * width * hidden,
            bytes_accessed=tokens_all * width * 8,
            transcendentals=blocks * locals_ * slots * hidden,
        ),
        name="experts",
    )(place, x_all, g_all, rank, router_rows, *gate_parts, *up_parts, w_down)
    return got[0], got[1], got[2], got[3 : 3 + shards], got[3 + shards :]


def split_columns(me, weights, shards):
    locals_, rows, width = weights[0].shape
    part = width // shards

    def kernel(place_ref, *refs):
        count = len(refs) // 2
        for i in range(count):
            refs[count + i][...] = refs[i][...]

    def block(k):
        return pl.BlockSpec((1, rows, part), lambda e, at: (e, 0, lax.rem(at[0] + k, shards)))

    got = pl.pallas_call(
        kernel,
        grid_spec=pltpu.PrefetchScalarGridSpec(
            num_scalar_prefetch=1,
            grid=(locals_,),
            in_specs=[block(k) for _ in weights for k in range(shards)],
            out_specs=[pl.BlockSpec((1, rows, part), lambda e, at: (e, 0, 0))]
            * (len(weights) * shards),
        ),
        out_shape=[jax.ShapeDtypeStruct((locals_, rows, part), weights[0].dtype)]
        * (len(weights) * shards),
        cost_estimate=pl.CostEstimate(
            flops=0, bytes_accessed=4 * len(weights) * locals_ * rows * width, transcendentals=0
        ),
        name="split_columns",
    )(me, *[w for w in weights for _ in range(shards)])
    return [got[i * shards : (i + 1) * shards] for i in range(len(weights))]


def join_columns(me, parts):
    shards = len(parts)
    locals_, hidden, rows = parts[0].shape

    def kernel(place_ref, *refs):
        out_ref = refs[shards]
        for k in range(shards):

            @pl.when(pl.program_id(1) == k)
            def _():
                out_ref[0] = refs[k][0].astype(jnp.float32).T

    return pl.pallas_call(
        kernel,
        grid_spec=pltpu.PrefetchScalarGridSpec(
            num_scalar_prefetch=1,
            grid=(locals_, shards),
            in_specs=[pl.BlockSpec((1, hidden, rows), lambda e, k, at: (e, 0, 0))] * shards,
            out_specs=pl.BlockSpec(
                (1, rows, hidden), lambda e, k, at: (e, 0, lax.rem(at[0] + shards - k, shards))
            ),
        ),
        out_shape=jax.ShapeDtypeStruct((locals_, rows, shards * hidden), jnp.float32),
        cost_estimate=pl.CostEstimate(
            flops=0, bytes_accessed=6 * locals_ * rows * shards * hidden, transcendentals=0
        ),
        name="join_columns",
    )(me, *parts)


def shifted(values, count, step):
    return lax.ppermute(values, "fs", [(i, (i + step) % count) for i in range(count)])


def fs_exchange(pieces):
    count = pieces.shape[0]
    me = lax.axis_index("fs")
    result = jnp.zeros_like(pieces)
    result = lax.dynamic_update_index_in_dim(
        result, lax.dynamic_index_in_dim(pieces, me, 0, False), me, 0
    )
    for step in range(1, count):
        sent = lax.dynamic_index_in_dim(pieces, (me + step) % count, 0, False)
        result = lax.dynamic_update_index_in_dim(
            result, shifted(sent, count, step), (me - step) % count, 0
        )
    return result


def fs_gather(values):
    count = lax.axis_size("fs")
    me = lax.axis_index("fs")
    result = jnp.zeros((count,) + values.shape, values.dtype)
    for step in range(count):
        got = shifted(values, count, step) if step else values
        result = lax.dynamic_update_index_in_dim(result, got, (me - step) % count, 0)
    return result


def fs_sum(partial):
    count = lax.axis_size("fs")
    me = lax.axis_index("fs")
    rows = partial.shape[0] // count
    own = lax.dynamic_slice_in_dim(partial, me * rows, rows).astype(jnp.float32)
    for step in range(1, count):
        sent = lax.dynamic_slice_in_dim(partial, ((me + step) % count) * rows, rows)
        own = own + shifted(sent.astype(low_type), count, step).astype(jnp.float32)
    return own


def fs_send(parts):
    count = len(parts)
    return [parts[0]] + [shifted(parts[k], count, k) for k in range(1, count)]


def ep_flip(values, bit):
    count = lax.axis_size("ep")
    return lax.ppermute(values, "ep", [(i, i ^ (1 << bit)) for i in range(count)])


def ep_gather(values):
    bits = lax.axis_size("ep").bit_length() - 1
    me = lax.axis_index("ep")
    held = values
    order = range(bits - 1, -1, -1)
    for bit in order:
        got = ep_flip(held, bit)
        low = ((me >> bit) & 1) == 0
        held = jnp.stack([jnp.where(low, held, got), jnp.where(low, got, held)])
    held = jnp.transpose(held, (*range(bits - 1, -1, -1), *range(bits, held.ndim)))
    return held.reshape((1 << bits,) + values.shape)


def ep_sum(partial, after=None):
    count = lax.axis_size("ep")
    bits = count.bit_length() - 1
    me = lax.axis_index("ep")
    rows, columns = partial.shape[0] // count, partial.shape[1]

    if after is not None:
        me = me + (after[0, 0].astype(jnp.float32) * 0.0).astype(jnp.int32)

    def halve(held, bit, axis):
        mine = (me >> bit) & 1
        got = ep_flip(lax.dynamic_index_in_dim(held, 1 - mine, axis, False), bit)
        kept = lax.dynamic_index_in_dim(held, mine, axis, False)
        return (kept.astype(jnp.float32) + got.astype(jnp.float32)).astype(low_type)

    first = halve(partial.reshape(count // 2, 2, rows, columns), 0, 1)
    half = columns // 2 // 128 * 128
    results = []
    for start, stop, order in (
        (0, half, range(1, bits)),
        (half, columns, range(bits - 1, 0, -1)),
    ):
        held = first[:, :, start:stop].reshape((2,) * (bits - 1) + (rows, stop - start))
        left = list(range(bits - 1, 0, -1))
        for bit in order:
            held = halve(held, bit, left.index(bit))
            left.remove(bit)
        results.append(held)
    return jnp.concatenate(results, axis=1)


def on_device(
    tokens,
    attn_gain,
    w_query,
    w_key,
    w_value,
    query_gain,
    key_gain,
    w_output,
    ffn_gain,
    w_router,
    w_gate,
    w_up,
    w_down,
    seq_lengths,
    span_places,
    routes,
    out_grad,
):
    rows_dev, width = tokens.shape
    n_fs = lax.axis_size("fs")
    n_ep = lax.axis_size("ep")
    devices = n_fs * n_ep
    fs_at = lax.axis_index("fs")
    ep_at = lax.axis_index("ep")
    group_rows = rows_dev * n_fs
    shard_rows = width // n_fs
    head_dim = query_gain.shape[0] * n_fs
    head_width = width // n_fs
    local_experts = w_gate.shape[0]
    experts_total = local_experts * n_ep
    top_count = routes.shape[1]
    hidden = w_gate.shape[2] // n_fs
    capacity = 4 * rows_dev * top_count // (3 * experts_total)

    tokens_group = lax.all_gather(tokens, "fs", axis=0, tiled=True)
    small = jnp.concatenate(
        [w_router.reshape(-1), attn_gain, ffn_gain, query_gain, key_gain], axis=0
    )
    small = fs_gather(small)
    cut = shard_rows * experts_total
    router_full = small[:, :cut].reshape(width, experts_total)
    gain_one = small[:, cut : cut + shard_rows].reshape(width).astype(jnp.float32)
    cut += shard_rows
    gain_two = small[:, cut : cut + shard_rows].reshape(width).astype(jnp.float32)
    cut += shard_rows
    part = head_dim // n_fs
    gain_query = small[:, cut : cut + part].reshape(1, head_dim).astype(jnp.float32)
    cut += part
    gain_key = small[:, cut : cut + part].reshape(1, head_dim).astype(jnp.float32)

    share = shard_rows // n_ep
    heads_in = jnp.stack(
        [
            lax.dynamic_slice_in_dim(w, ep_at * share, share).reshape(share, n_fs, head_width)
            for w in (w_query, w_key, w_value)
        ],
        axis=2,
    )
    heads_in = fs_exchange(jnp.transpose(heads_in, (1, 0, 2, 3)))
    heads_in = ep_gather(heads_in)
    w_heads = jnp.transpose(heads_in, (1, 0, 2, 3, 4)).reshape(width, 3 * head_width)

    fs_place = fs_at.reshape(1).astype(jnp.int32)
    gate_send, up_send = split_columns(fs_place, (w_gate, w_up), n_fs)
    gate_parts = fs_send(gate_send)
    up_parts = fs_send(up_send)

    expert_ids = jnp.arange(experts_total, dtype=jnp.int32)
    hit = jnp.any(routes[:, :, None] == expert_ids[None, None, :], axis=1)
    before = jnp.arange(rows_dev, dtype=jnp.int32)
    upper = (before[:, None] <= before[None, :]).astype(low_type)
    counts = mm(hit.astype(low_type), upper, TN)
    rank = jnp.where(hit.T, counts.astype(jnp.int32) - 1, -1)
    wide = jnp.concatenate([out_grad, rank.T.astype(low_type)], axis=1)
    wide = jnp.pad(wide, ((0, 0), (0, 128 - experts_total)))
    grad_all = lax.all_gather(wide, ("ep", "fs"), axis=0, tiled=True)
    base = ep_at * local_experts
    rank_all = jnp.transpose(
        grad_all[:, width : width + experts_total].reshape(devices, rows_dev, experts_total),
        (0, 2, 1),
    ).astype(jnp.int32)
    rank_rolled = jnp.roll(rank_all, -base, axis=1)
    router_rows = jnp.roll(router_full.T, -base, axis=0)

    segment, position = group_layout(
        seq_lengths[0], span_places[0], group_rows, group_rows // span_places.shape[1]
    )
    half_dim = head_dim // 2
    inverse = jnp.exp(
        jnp.arange(half_dim).astype(jnp.float32) * (-2.0 * math.log(rope_base) / head_dim)
    )
    angles = position.astype(jnp.float32)[:, None] * inverse[None, :]
    cosines = jnp.cos(angles)
    sines = jnp.sin(angles)
    cos2 = jnp.concatenate([cosines, cosines], axis=1)
    sin2 = jnp.concatenate([-sines, sines], axis=1)
    group_in = tokens_group.astype(jnp.float32)
    group_scale = rms_scale(group_in)
    normed_group = (group_in * group_scale * gain_one).astype(low_type)
    qkv = mm(normed_group, w_heads, NN)
    attended = attention_forward(qkv, gain_query, gain_key, cos2, sin2, segment, head_dim)
    branch = fs_sum(mm(attended, w_output, NN).astype(low_type))
    hidden_in = tokens.astype(jnp.float32)
    scale_one = rms_scale(hidden_in)
    hidden_mid = hidden_in + branch
    scale_two = rms_scale(hidden_mid)
    normed_two = (hidden_mid * scale_two * gain_two).astype(low_type)

    normed_all = lax.all_gather(normed_two, ("ep", "fs"), axis=0, tiled=True)
    out_part, dx_part, dwd, dwg, dwu = run_experts(
        jnp.stack([base, fs_at]).astype(jnp.int32),
        normed_all,
        grad_all,
        rank_rolled,
        router_rows,
        gate_parts,
        up_parts,
        w_down,
        capacity,
    )
    dx_group = ep_sum(dx_part)
    dx_own = fs_sum(dx_group)
    gate_grad = join_columns(fs_place, fs_send(dwg))
    up_grad = join_columns(fs_place, fs_send(dwu))

    logits = mm(normed_two, router_full, NN)
    kept = jnp.where(hit, logits, -1e30)
    powers = jnp.where(hit, jnp.exp(kept - jnp.max(kept, axis=1, keepdims=True)), 0.0)
    gates = powers / jnp.sum(powers, axis=1, keepdims=True)
    grad_gates = (
        dx_own[:, width : width + experts_total]
        + dx_own[:, width + experts_total : width + 2 * experts_total]
    )
    weighted = gates * grad_gates
    grad_logits = (weighted - gates * jnp.sum(weighted, axis=1, keepdims=True)).astype(low_type)
    router_grad = mm(normed_two, grad_logits, TN)
    grad_normed_two = dx_own[:, :width] + mm(grad_logits, router_full, NT)
    grad_mid_norm, gain_two_terms = norm_back(hidden_mid, scale_two, gain_two, grad_normed_two)
    gain_two_grad = jnp.sum(gain_two_terms, axis=0)
    grad_mid = out_grad.astype(jnp.float32) + grad_mid_norm

    branch_group = lax.all_gather(grad_mid.astype(low_type), "fs", axis=0, tiled=True)
    grad_attended = mm(branch_group, w_output, NT).astype(low_type)
    output_w_grad = mm(attended, branch_group, TN).astype(low_type)
    dq, dk, dv, dgq, dgk = attention_backward(
        qkv, grad_attended, gain_query, gain_key, cos2, sin2, segment, head_dim
    )
    grad_qkv = jnp.concatenate([dq, dk, dv], axis=1)
    heads_w_grad = mm(normed_group, grad_qkv, TN).astype(low_type)
    grad_normed_part = mm(grad_qkv, w_heads, NT)
    gain_one_grad = jnp.sum(grad_normed_part * group_in * group_scale, axis=0)
    grad_normed_one = fs_sum(grad_normed_part.astype(low_type))
    grad_in_norm, _ = norm_back(hidden_in, scale_one, gain_one, grad_normed_one)
    tokens_grad = (grad_mid + grad_in_norm).astype(low_type)

    out_w = lax.psum_scatter(output_w_grad, "ep", scatter_dimension=0, tiled=True)
    out_w = lax.ppermute(
        out_w,
        ("ep", "fs"),
        [(e * n_fs + z, z * n_ep + e) for e in range(n_ep) for z in range(n_fs)],
    ).astype(jnp.float32)
    heads_w = lax.psum_scatter(heads_w_grad, "ep", scatter_dimension=0, tiled=True)
    heads_w = fs_exchange(heads_w.reshape(n_fs, width // devices, 3 * head_width))
    heads_w = jnp.transpose(
        heads_w.reshape(n_fs, width // devices, 3, head_width), (2, 1, 0, 3)
    ).reshape(3, width // devices, width).astype(jnp.float32)

    def spread(values):
        each = head_dim // devices
        return jnp.pad(values.reshape(devices, each), ((0, 0), (0, width // devices - each))).reshape(
            width, 1
        )

    sums = jnp.concatenate(
        [
            router_grad,
            gain_two_grad[:, None],
            gain_one_grad[:, None],
            spread(jnp.sum(dgq, axis=(0, 1))),
            spread(jnp.sum(dgk, axis=(0, 1))),
        ],
        axis=1,
    )
    sums = jnp.pad(sums, ((0, 0), (0, 128 - sums.shape[1])))
    sums = lax.psum_scatter(sums, ("ep", "fs"), scatter_dimension=0, tiled=True)
    each = head_dim // devices

    out_group = ep_sum(out_part, dx_group)
    output = (hidden_mid + fs_sum(out_group)).astype(low_type)
    return (
        output,
        tokens_grad,
        sums[:, experts_total + 1],
        heads_w[0],
        heads_w[1],
        heads_w[2],
        sums[:each, experts_total + 2],
        sums[:each, experts_total + 3],
        out_w,
        sums[:, experts_total],
        sums[:, :experts_total],
        gate_grad,
        up_grad,
        dwd,
    )


def solution(mesh):
    return jax.shard_map(
        on_device,
        mesh=mesh,
        in_specs=(
            P(("ep", "fs"), None),
            P("fs"),
            P("fs", None),
            P("fs", None),
            P("fs", None),
            P("fs"),
            P("fs"),
            P("fs", None),
            P("fs"),
            P("fs", None),
            P("ep", "fs", None),
            P("ep", "fs", None),
            P("ep", "fs", None),
            P("ep", None),
            P("ep", None),
            P(("ep", "fs"), None),
            P(("ep", "fs"), None),
        ),
        out_specs=(
            P(("ep", "fs"), None),
            P(("ep", "fs"), None),
            P(("ep", "fs")),
            P(("ep", "fs"), None),
            P(("ep", "fs"), None),
            P(("ep", "fs"), None),
            P(("ep", "fs")),
            P(("ep", "fs")),
            P(("ep", "fs"), None),
            P(("ep", "fs")),
            P(("ep", "fs"), None),
            P("ep", "fs", None),
            P("ep", "fs", None),
            P("ep", "fs", None),
        ),
        check_vma=False,
    )
```

```python
import math

import jax
import jax.numpy as jnp
from jax import lax
from jax.experimental import pallas as pl
from jax.experimental.pallas import tpu as pltpu
from jax.sharding import PartitionSpec as P

epsilon = 1e-06
rope_base = 10000.0
masked_score = -1000000000.0
low_type = jnp.bfloat16
VMEM_LIMIT = 66_000_000


def rms_scale(values):
    return lax.rsqrt(jnp.mean(values * values, axis=-1, keepdims=True) + epsilon)


def mm(a, b, dims):
    return lax.dot_general(a, b, (dims, ((), ())), preferred_element_type=jnp.float32)


NN = ((1,), (0,))
NT = ((1,), (1,))
TN = ((0,), (0,))


def norm_back(values, scale, gain, upstream):
    weighted = upstream * gain
    inner_mean = jnp.mean(weighted * values, axis=-1, keepdims=True)
    return (
        scale * weighted - values * (scale * scale * scale) * inner_mean,
        upstream * values * scale,
    )


def group_layout(lengths_row, places_row, group_rows, span_rows):
    arrival = jnp.arange(group_rows, dtype=jnp.int32)
    span_hit = (arrival // span_rows)[:, None] == jnp.arange(places_row.shape[0], dtype=jnp.int32)[
        None, :
    ]
    places = (
        jnp.sum(jnp.where(span_hit, places_row[None, :], 0), axis=1) * span_rows
        + arrival % span_rows
    )
    seq_ends = jnp.cumsum(lengths_row)
    segment = jnp.sum((places[:, None] >= seq_ends[None, :]).astype(jnp.int32), axis=1)
    seq_starts = seq_ends - lengths_row
    picked = segment[:, None] == jnp.arange(lengths_row.shape[0], dtype=jnp.int32)[None, :]
    position = places - jnp.sum(jnp.where(picked, seq_starts[None, :], 0), axis=1)
    return (segment, position)


def rotated(pre, gain, cos2, sin2):
    scale = rms_scale(pre)
    normed = pre * scale * gain
    half = pre.shape[1] // 2
    return scale, normed * cos2 + pltpu.roll(normed, half, 1) * sin2


def attn_forward_kernel(
    q_ref, k_ref, v_ref, gq_ref, gk_ref, cos_ref, sin_ref, segc_ref, segr_ref, o_ref, q_scr, *, block
):
    rows = q_ref.shape[0]
    factor = 1.0 / math.sqrt(q_ref.shape[1])
    cos2 = cos_ref[...]
    sin2 = sin_ref[...]
    q_scr[...] = rotated(q_ref[...], gq_ref[...], cos2, sin2)[1].astype(low_type)
    key = rotated(k_ref[...], gk_ref[...], cos2, sin2)[1].astype(low_type)
    value = v_ref[...].astype(low_type)

    def step(i, carry):
        at = pl.ds(pl.multiple_of(i * block, block), block)
        raw = mm(q_scr[at, :], key, NT) * factor
        raw = jnp.where(segc_ref[at, :] == segr_ref[...], raw, masked_score)
        peak = jnp.max(raw, axis=1, keepdims=True)
        powers = jnp.exp(raw - peak)
        weights = powers / jnp.sum(powers, axis=1, keepdims=True)
        o_ref[at, :] = mm(weights.astype(low_type), value, NN).astype(low_type)
        return carry

    lax.fori_loop(0, rows // block, step, 0)


def attn_backward_kernel(
    q_ref,
    k_ref,
    v_ref,
    da_ref,
    gq_ref,
    gk_ref,
    cos_ref,
    sin_ref,
    segc_ref,
    segr_ref,
    dq_ref,
    dk_ref,
    dv_ref,
    dgq_ref,
    dgk_ref,
    q_scr,
    dq_scr,
    dk_scr,
    dv_scr,
    *,
    block,
):
    rows, head_dim = q_ref.shape
    factor = 1.0 / math.sqrt(head_dim)
    cos2 = cos_ref[...]
    sin2 = sin_ref[...]
    q_scale, q_rot = rotated(q_ref[...], gq_ref[...], cos2, sin2)
    q_scr[...] = q_rot.astype(low_type)
    k_scale, k_rot = rotated(k_ref[...], gk_ref[...], cos2, sin2)
    key = k_rot.astype(low_type)
    value = v_ref[...].astype(low_type)
    dk_scr[...] = jnp.zeros_like(dk_scr)
    dv_scr[...] = jnp.zeros_like(dv_scr)

    def step(i, carry):
        at = pl.ds(pl.multiple_of(i * block, block), block)
        query = q_scr[at, :]
        grads = da_ref[at, :]
        raw = mm(query, key, NT) * factor
        raw = jnp.where(segc_ref[at, :] == segr_ref[...], raw, masked_score)
        peak = jnp.max(raw, axis=1, keepdims=True)
        powers = jnp.exp(raw - peak)
        probs = powers / jnp.sum(powers, axis=1, keepdims=True)
        grad_probs = mm(grads, value, NT)
        delta = jnp.sum(probs * grad_probs, axis=1, keepdims=True)
        grad_scores = (probs * (grad_probs - delta)).astype(low_type)
        dq_scr[at, :] = mm(grad_scores, key, NN) * factor
        dk_scr[...] += mm(grad_scores, query, TN)
        dv_scr[...] += mm(probs.astype(low_type), grads, TN)
        return carry

    lax.fori_loop(0, rows // block, step, 0)
    half = head_dim // 2

    def finish(pre, scale, gain, upstream, out_ref, gain_out_ref):
        upstream = upstream.astype(low_type).astype(jnp.float32)
        back = upstream * cos2 - pltpu.roll(upstream, half, 1) * sin2
        grad_pre, gain_terms = norm_back(pre, scale, gain, back)
        out_ref[...] = grad_pre.astype(low_type)
        gain_out_ref[0] = jnp.sum(gain_terms, axis=0, keepdims=True)

    finish(q_ref[...], q_scale, gq_ref[...], dq_scr[...], dq_ref, dgq_ref)
    finish(k_ref[...], k_scale, gk_ref[...], dk_scr[...] * factor, dk_ref, dgk_ref)
    dv_ref[...] = dv_scr[...].astype(low_type)


def attention_forward(qkv, gain_q, gain_k, cos2, sin2, segment, head_dim):
    rows, width3 = qkv.shape
    heads = width3 // (3 * head_dim)
    block = 256
    col = lambda part: pl.BlockSpec((rows, head_dim), lambda h: (0, part * heads + h))
    full = lambda shape: pl.BlockSpec(shape, lambda h: (0, 0))
    return pl.pallas_call(
        lambda *refs: attn_forward_kernel(*refs, block=block),
        grid=(heads,),
        in_specs=[
            col(0),
            col(1),
            col(2),
            full((1, head_dim)),
            full((1, head_dim)),
            full((rows, head_dim)),
            full((rows, head_dim)),
            full((rows, 1)),
            full((1, rows)),
        ],
        out_specs=pl.BlockSpec((rows, head_dim), lambda h: (0, h)),
        out_shape=jax.ShapeDtypeStruct((rows, heads * head_dim), low_type),
        scratch_shapes=[pltpu.VMEM((rows, head_dim), low_type)],
        compiler_params=pltpu.CompilerParams(vmem_limit_bytes=VMEM_LIMIT // 2),
        cost_estimate=pl.CostEstimate(
            flops=heads * rows * rows * head_dim * 4,
            bytes_accessed=rows * width3 * 4,
            transcendentals=heads * rows * rows,
        ),
        name="attn_forward",
    )(qkv, qkv, qkv, gain_q, gain_k, cos2, sin2, segment[:, None], segment[None, :])


def attention_backward(qkv, grad_attended, gain_q, gain_k, cos2, sin2, segment, head_dim):
    rows, width3 = qkv.shape
    heads = width3 // (3 * head_dim)
    block = 256
    col = lambda part: pl.BlockSpec((rows, head_dim), lambda h: (0, part * heads + h))
    full = lambda shape: pl.BlockSpec(shape, lambda h: (0, 0))
    wide = jax.ShapeDtypeStruct((rows, heads * head_dim), low_type)
    gain = jax.ShapeDtypeStruct((heads, 1, head_dim), jnp.float32)
    gain_spec = pl.BlockSpec((1, 1, head_dim), lambda h: (h, 0, 0))
    return pl.pallas_call(
        lambda *refs: attn_backward_kernel(*refs, block=block),
        grid=(heads,),
        in_specs=[
            col(0),
            col(1),
            col(2),
            col(0),
            full((1, head_dim)),
            full((1, head_dim)),
            full((rows, head_dim)),
            full((rows, head_dim)),
            full((rows, 1)),
            full((1, rows)),
        ],
        out_specs=[col(0), col(0), col(0), gain_spec, gain_spec],
        out_shape=[wide, wide, wide, gain, gain],
        scratch_shapes=[
            pltpu.VMEM((rows, head_dim), low_type),
            pltpu.VMEM((rows, head_dim), jnp.float32),
            pltpu.VMEM((rows, head_dim), jnp.float32),
            pltpu.VMEM((rows, head_dim), jnp.float32),
        ],
        compiler_params=pltpu.CompilerParams(vmem_limit_bytes=VMEM_LIMIT // 2),
        cost_estimate=pl.CostEstimate(
            flops=heads * rows * rows * head_dim * 10,
            bytes_accessed=rows * width3 * 6,
            transcendentals=heads * rows * rows,
        ),
        name="attn_backward",
    )(qkv, qkv, qkv, grad_attended, gain_q, gain_k, cos2, sin2, segment[:, None], segment[None, :])


def experts_kernel(place_ref, *refs, sources, cap, locals_, total, shards):
    x_ref, g_ref, rank_ref, router_ref = refs[:4]
    refs = refs[4:]
    gate_refs, up_refs, wd_ref = refs[:shards], refs[shards : 2 * shards], refs[2 * shards]
    refs = refs[2 * shards + 1 :]
    out_hbm, dx_kept, dx_sent, dwd_hbm = refs[:4]
    dwg_hbm, dwu_hbm = refs[4 : 4 + shards], refs[4 + shards : 4 + 2 * shards]
    refs = refs[4 + 2 * shards :]
    x_slots, g_slots, gates_col, acc_g, acc_u, acc_d, out_stage, dx_stage = refs[:8]
    out_sem, dx_sem, acc_sem, grad_sem = refs[8:]
    b = pl.program_id(0)
    e = pl.program_id(1)
    blocks = pl.num_programs(0)
    rows = x_ref.shape[0] // sources
    width = x_ref.shape[1]
    chunk = width // shards
    slots = sources * cap
    me = place_ref[1]

    def one_hot(s):
        slot = lax.broadcasted_iota(jnp.int32, (cap, rows), 0)
        return [slot == rank_ref[s, j : j + 1, :] for j in range(locals_)]

    @pl.when(e == 0)
    def _():
        for s in range(sources):
            at = pl.ds(s * rows, rows)
            logits = mm(router_ref[...], x_ref[at, :], NT)
            live = rank_ref[s] >= 0
            kept = jnp.where(live, logits, -1e30)
            powers = jnp.where(live, jnp.exp(kept - jnp.max(kept, axis=0, keepdims=True)), 0.0)
            gates = powers / jnp.sum(powers, axis=0, keepdims=True)
            hits = one_hot(s)
            for j in range(locals_):
                picked = jnp.sum(
                    jnp.where(hits[j], gates[j : j + 1, :], 0.0), axis=1, keepdims=True
                )
                gates_col[j, s * cap : (s + 1) * cap, :] = jnp.broadcast_to(
                    picked, (cap, gates_col.shape[2])
                )
            select = jnp.concatenate([h.astype(jnp.float32) for h in hits], axis=0).astype(low_type)
            for c in range(0, width, chunk):
                picked_x = mm(select, x_ref[at, c : c + chunk], NN).astype(low_type)
                picked_g = mm(select, g_ref[at, c : c + chunk], NN).astype(low_type)
                for j in range(locals_):
                    x_slots[j, s * cap : (s + 1) * cap, c : c + chunk] = picked_x[
                        j * cap : (j + 1) * cap
                    ]
                    g_slots[j, s * cap : (s + 1) * cap, c : c + chunk] = picked_g[
                        j * cap : (j + 1) * cap
                    ]

    @pl.when(b == 0)
    def _():
        acc_g[e] = jnp.zeros(acc_g.shape[1:], jnp.float32)
        acc_u[e] = jnp.zeros(acc_u.shape[1:], jnp.float32)
        acc_d[e] = jnp.zeros(acc_d.shape[1:], jnp.float32)

    hidden = wd_ref.shape[1]
    gate = gates_col[e][:, :1]
    gs = g_slots[e, :slots, :width]
    gate_pre = jnp.zeros((slots, hidden), jnp.float32)
    up_pre = jnp.zeros((slots, hidden), jnp.float32)
    columns = [
        pl.ds(pl.multiple_of(lax.rem(me + shards - k, shards) * chunk, chunk), chunk)
        for k in range(shards)
    ]
    for k in range(shards):
        xs = x_slots[e, :slots, columns[k]]
        gate_pre += mm(xs, gate_refs[k][0], NN)
        up_pre += mm(xs, up_refs[k][0], NN)
    back = mm(gs, wd_ref[0], NT)
    sigmoid = jax.nn.sigmoid(gate_pre)
    silu = gate_pre * sigmoid
    activated = silu * up_pre
    grad_gate_dot = jnp.sum(
        activated.astype(low_type).astype(jnp.float32) * back, axis=1, keepdims=True
    )
    grad_act = back * gate
    grad_up = (grad_act * silu).astype(low_type)
    grad_gate = (grad_act * up_pre * sigmoid * (1.0 + gate_pre * (1.0 - sigmoid))).astype(low_type)
    act_gated = (activated * gate).astype(low_type)
    for c in range(0, width, chunk):
        cols = pl.ds(c, chunk)
        acc_g[e, :, cols] += mm(grad_gate, x_slots[e, :slots, cols], TN)
        acc_u[e, :, cols] += mm(grad_up, x_slots[e, :slots, cols], TN)
        acc_d[e, :, cols] += mm(act_gated, g_slots[e, :slots, cols], TN)
    for c in range(0, width, chunk):
        cols = pl.ds(c, chunk)
        x_slots[e, :slots, cols] = mm(act_gated, wd_ref[0, :, cols], NN).astype(low_type)
    for k in range(shards):
        g_slots[e, :slots, columns[k]] = (
            mm(grad_gate, gate_refs[k][0], NT) + mm(grad_up, up_refs[k][0], NT)
        ).astype(low_type)
    lanes = g_slots.shape[2] - width
    lane = lax.broadcasted_iota(jnp.int32, (slots, lanes), 1)
    high = grad_gate_dot.astype(low_type).astype(jnp.float32)
    mine = place_ref[0] + e
    g_slots[e, :slots, width:] = jnp.where(
        lane == mine, high, jnp.where(lane == mine + total, grad_gate_dot - high, 0.0)
    ).astype(low_type)

    @pl.when(e == pl.num_programs(1) - 1)
    def _():
        pending = [None, None]
        for s in range(sources):
            slot = s % 2
            if pending[slot] is not None:
                for copy in pending[slot]:
                    copy.wait()
            hits = one_hot(s)
            select = jnp.concatenate([h.astype(jnp.float32) for h in hits], axis=0).astype(low_type)
            part = slice(s * cap, (s + 1) * cap)
            for c in range(0, width, chunk):
                cols = slice(c, c + chunk)
                ys = jnp.concatenate([x_slots[j, part, cols] for j in range(locals_)], axis=0)
                out_stage[slot, :, cols] = mm(select, ys, TN).astype(low_type)
                ds_ = jnp.concatenate([g_slots[j, part, cols] for j in range(locals_)], axis=0)
                dx_stage[slot, :, cols] = mm(select, ds_, TN).astype(low_type)
            tail = jnp.concatenate([g_slots[j, part, width:] for j in range(locals_)], axis=0)
            dx_stage[slot, :, width:] = mm(select, tail, TN).astype(low_type)
            number = b * sources + s
            group = lax.div(number, shards)
            within = number - group * shards
            at = pl.ds(number * rows, rows)
            to = pl.ds((lax.div(group, 2) * shards + within) * rows, rows)
            copies = (
                pltpu.make_async_copy(out_stage.at[slot], out_hbm.at[at], out_sem.at[slot]),
                pltpu.make_async_copy(dx_stage.at[slot], dx_kept.at[to], dx_sem.at[slot]),
            )
            copies[0].start()
            mine_too = lax.rem(group, 2) == place_ref[2]

            @pl.when(mine_too)
            def _():
                copies[1].start()

            @pl.when(jnp.logical_not(mine_too))
            def _():
                pltpu.make_async_copy(dx_stage.at[slot], dx_sent.at[to], dx_sem.at[slot]).start()

            pending[slot] = copies
        for copies in pending:
            if copies is not None:
                for copy in copies:
                    copy.wait()

    @pl.when((b == blocks - 1) & (e == locals_ - 1))
    def _():
        copies = [pltpu.make_async_copy(acc_d, dwd_hbm, acc_sem)]
        copies[0].start()
        for j in range(locals_):
            x_slots[j, :hidden, :] = acc_g[j].astype(low_type)
            g_slots[j, :hidden, :width] = acc_u[j].astype(low_type)
            for k in range(shards):
                cols = pl.ds(pl.multiple_of(lax.rem(me + k, shards) * chunk, chunk), chunk)
                for which, (held, target) in enumerate(((x_slots, dwg_hbm), (g_slots, dwu_hbm))):
                    copy = pltpu.make_async_copy(
                        held.at[j, pl.ds(0, hidden), cols],
                        target[k].at[j],
                        grad_sem.at[which, j, k],
                    )
                    copy.start()
                    copies.append(copy)
        for copy in copies:
            copy.wait()


def run_experts(place, x_all, g_all, rank, router_rows, gate_parts, up_parts, w_down, cap):
    tokens_all, width = x_all.shape
    devices, total, rows = rank.shape
    shards = len(gate_parts)
    locals_, shard_rows, hidden = gate_parts[0].shape
    sources = 4
    blocks = devices // sources
    block_rows = sources * rows
    slots = sources * cap
    held_rows = max(slots, hidden)
    any_spec = pl.BlockSpec(memory_space=pl.ANY)
    weight_spec = pl.BlockSpec((1, shard_rows, hidden), lambda b, e, *_: (e, 0, 0))
    grid_spec = pltpu.PrefetchScalarGridSpec(
        num_scalar_prefetch=1,
        grid=(blocks, locals_),
        in_specs=[
            pl.BlockSpec((block_rows, width), lambda b, e, *_: (b, 0)),
            pl.BlockSpec((block_rows, width), lambda b, e, *_: (b, 0)),
            pl.BlockSpec((sources, total, rows), lambda b, e, *_: (b, 0, 0)),
            pl.BlockSpec((total, width), lambda b, e, *_: (0, 0)),
            *([weight_spec] * (2 * shards)),
            pl.BlockSpec((1, hidden, width), lambda b, e, *_: (e, 0, 0)),
        ],
        out_specs=[any_spec] * (4 + 2 * shards),
        scratch_shapes=[
            pltpu.VMEM((locals_, held_rows, width), low_type),
            pltpu.VMEM((locals_, held_rows, width + 128), low_type),
            pltpu.VMEM((locals_, slots, 128), jnp.float32),
            pltpu.VMEM((locals_, hidden, width), jnp.float32),
            pltpu.VMEM((locals_, hidden, width), jnp.float32),
            pltpu.VMEM((locals_, hidden, width), jnp.float32),
            pltpu.VMEM((2, rows, width), low_type),
            pltpu.VMEM((2, rows, width + 128), low_type),
            pltpu.SemaphoreType.DMA((2,)),
            pltpu.SemaphoreType.DMA((2,)),
            pltpu.SemaphoreType.DMA,
            pltpu.SemaphoreType.DMA((2, locals_, shards)),
        ],
    )
    piece = jax.ShapeDtypeStruct((locals_, hidden, shard_rows), low_type)
    got = pl.pallas_call(
        lambda *refs: experts_kernel(
            *refs, sources=sources, cap=cap, locals_=locals_, total=total, shards=shards
        ),
        grid_spec=grid_spec,
        out_shape=[
            jax.ShapeDtypeStruct((tokens_all, width), low_type),
            jax.ShapeDtypeStruct((tokens_all // 2, width + 128), low_type),
            jax.ShapeDtypeStruct((tokens_all // 2, width + 128), low_type),
            jax.ShapeDtypeStruct((locals_, hidden, width), jnp.float32),
            *([piece] * (2 * shards)),
        ],
        input_output_aliases={1: 0},
        compiler_params=pltpu.CompilerParams(vmem_limit_bytes=VMEM_LIMIT),
        cost_estimate=pl.CostEstimate(
            flops=18 * blocks * locals_ * slots * width * hidden,
            bytes_accessed=tokens_all * width * 8,
            transcendentals=blocks * locals_ * slots * hidden,
        ),
        name="experts",
    )(place, x_all, g_all, rank, router_rows, *gate_parts, *up_parts, w_down)
    return got[:4], got[4 : 4 + shards], got[4 + shards :]


def split_columns(me, weights, shards):
    locals_, rows, width = weights[0].shape
    part = width // shards

    def kernel(place_ref, *refs):
        count = len(refs) // 2
        for i in range(count):
            refs[count + i][...] = refs[i][...]

    def block(k):
        return pl.BlockSpec((1, rows, part), lambda e, at: (e, 0, lax.rem(at[0] + k, shards)))

    got = pl.pallas_call(
        kernel,
        grid_spec=pltpu.PrefetchScalarGridSpec(
            num_scalar_prefetch=1,
            grid=(locals_,),
            in_specs=[block(k) for _ in weights for k in range(shards)],
            out_specs=[pl.BlockSpec((1, rows, part), lambda e, at: (e, 0, 0))]
            * (len(weights) * shards),
        ),
        out_shape=[jax.ShapeDtypeStruct((locals_, rows, part), weights[0].dtype)]
        * (len(weights) * shards),
        cost_estimate=pl.CostEstimate(
            flops=0, bytes_accessed=4 * len(weights) * locals_ * rows * width, transcendentals=0
        ),
        name="split_columns",
    )(me, *[w for w in weights for _ in range(shards)])
    return [got[i * shards : (i + 1) * shards] for i in range(len(weights))]


def join_columns(me, parts):
    shards = len(parts)
    locals_, hidden, rows = parts[0].shape

    def kernel(place_ref, *refs):
        out_ref = refs[shards]
        for k in range(shards):

            @pl.when(pl.program_id(1) == k)
            def _():
                out_ref[0] = refs[k][0].astype(jnp.float32).T

    return pl.pallas_call(
        kernel,
        grid_spec=pltpu.PrefetchScalarGridSpec(
            num_scalar_prefetch=1,
            grid=(locals_, shards),
            in_specs=[pl.BlockSpec((1, hidden, rows), lambda e, k, at: (e, 0, 0))] * shards,
            out_specs=pl.BlockSpec(
                (1, rows, hidden), lambda e, k, at: (e, 0, lax.rem(at[0] + shards - k, shards))
            ),
        ),
        out_shape=jax.ShapeDtypeStruct((locals_, rows, shards * hidden), jnp.float32),
        cost_estimate=pl.CostEstimate(
            flops=0, bytes_accessed=6 * locals_ * rows * shards * hidden, transcendentals=0
        ),
        name="join_columns",
    )(me, *parts)


def shifted(values, count, step):
    return lax.ppermute(values, "fs", [(i, (i + step) % count) for i in range(count)])


def fs_exchange(pieces):
    count = pieces.shape[0]
    me = lax.axis_index("fs")
    result = jnp.zeros_like(pieces)
    result = lax.dynamic_update_index_in_dim(
        result, lax.dynamic_index_in_dim(pieces, me, 0, False), me, 0
    )
    for step in range(1, count):
        sent = lax.dynamic_index_in_dim(pieces, (me + step) % count, 0, False)
        result = lax.dynamic_update_index_in_dim(
            result, shifted(sent, count, step), (me - step) % count, 0
        )
    return result


def fs_gather(values):
    count = lax.axis_size("fs")
    me = lax.axis_index("fs")
    result = jnp.zeros((count,) + values.shape, values.dtype)
    for step in range(count):
        got = shifted(values, count, step) if step else values
        result = lax.dynamic_update_index_in_dim(result, got, (me - step) % count, 0)
    return result


def fs_sum(partial, after=(), wire=low_type):
    count = lax.axis_size("fs")
    me = tied(lax.axis_index("fs"), after)
    rows = partial.shape[0] // count
    own = lax.dynamic_slice_in_dim(partial, me * rows, rows).astype(jnp.float32)
    for step in range(1, count):
        sent = lax.dynamic_slice_in_dim(partial, ((me + step) % count) * rows, rows)
        own = own + shifted(sent.astype(wire), count, step).astype(jnp.float32)
    return own


def fs_send(parts):
    count = len(parts)
    return [parts[0]] + [shifted(parts[k], count, k) for k in range(1, count)]


def ep_flip(values, bit):
    count = lax.axis_size("ep")
    return lax.ppermute(values, "ep", [(i, i ^ (1 << bit)) for i in range(count)])


def ep_gather(values):
    bits = lax.axis_size("ep").bit_length() - 1
    me = lax.axis_index("ep")
    held = values
    order = range(bits - 1, -1, -1)
    for bit in order:
        got = ep_flip(held, bit)
        low = ((me >> bit) & 1) == 0
        held = jnp.stack([jnp.where(low, held, got), jnp.where(low, got, held)])
    held = jnp.transpose(held, (*range(bits - 1, -1, -1), *range(bits, held.ndim)))
    return held.reshape((1 << bits,) + values.shape)


def tied(number, arrays):
    for array in arrays:
        corner = lax.slice(array, (0,) * array.ndim, (1,) * array.ndim)
        number = number + (jnp.sum(corner.astype(jnp.float32)) * 0.0).astype(jnp.int32)
    return number


def ep_halve(kept, sent, bit):
    got = ep_flip(sent, bit)
    return (kept.astype(jnp.float32) + got.astype(jnp.float32)).astype(kept.dtype)


def ep_pick(held, bit, axis, me):
    mine = (me >> bit) & 1
    return (
        lax.dynamic_index_in_dim(held, mine, axis, False),
        lax.dynamic_index_in_dim(held, 1 - mine, axis, False),
    )


def ep_sum(partial, after=()):
    count = lax.axis_size("ep")
    me = tied(lax.axis_index("ep"), after)
    rows, columns = partial.shape[0] // count, partial.shape[1]
    kept, sent = ep_pick(partial.reshape(count // 2, 2, rows, columns), 0, 1, me)
    return ep_rest(ep_halve(kept, sent, 0), me)


def ep_rest(first, me):
    bits = lax.axis_size("ep").bit_length() - 1
    rows, columns = first.shape[1:]
    half = columns // 2 // 128 * 128
    results = []
    for start, stop, order in (
        (0, half, range(1, bits)),
        (half, columns, range(bits - 1, 0, -1)),
    ):
        if start == stop:
            continue
        held = first[:, :, start:stop].reshape((2,) * (bits - 1) + (rows, stop - start))
        left = list(range(bits - 1, 0, -1))
        for bit in order:
            held = ep_halve(*ep_pick(held, bit, left.index(bit), me), bit)
            left.remove(bit)
        results.append(held)
    return jnp.concatenate(results, axis=1) if len(results) > 1 else results[0]


def on_device(
    tokens,
    attn_gain,
    w_query,
    w_key,
    w_value,
    query_gain,
    key_gain,
    w_output,
    ffn_gain,
    w_router,
    w_gate,
    w_up,
    w_down,
    seq_lengths,
    span_places,
    routes,
    out_grad,
):
    rows_dev, width = tokens.shape
    n_fs = lax.axis_size("fs")
    n_ep = lax.axis_size("ep")
    devices = n_fs * n_ep
    fs_at = lax.axis_index("fs")
    ep_at = lax.axis_index("ep")
    group_rows = rows_dev * n_fs
    shard_rows = width // n_fs
    head_dim = query_gain.shape[0] * n_fs
    head_width = width // n_fs
    local_experts = w_gate.shape[0]
    experts_total = local_experts * n_ep
    top_count = routes.shape[1]
    hidden = w_gate.shape[2] // n_fs
    capacity = 4 * rows_dev * top_count // (3 * experts_total)

    tokens_group = lax.all_gather(tokens, "fs", axis=0, tiled=True)
    small = jnp.concatenate(
        [w_router.reshape(-1), attn_gain, ffn_gain, query_gain, key_gain], axis=0
    )
    small = fs_gather(small)
    cut = shard_rows * experts_total
    router_full = small[:, :cut].reshape(width, experts_total)
    gain_one = small[:, cut : cut + shard_rows].reshape(width).astype(jnp.float32)
    cut += shard_rows
    gain_two = small[:, cut : cut + shard_rows].reshape(width).astype(jnp.float32)
    cut += shard_rows
    part = head_dim // n_fs
    gain_query = small[:, cut : cut + part].reshape(1, head_dim).astype(jnp.float32)
    cut += part
    gain_key = small[:, cut : cut + part].reshape(1, head_dim).astype(jnp.float32)

    share = shard_rows // n_ep
    heads_in = jnp.stack(
        [
            lax.dynamic_slice_in_dim(w, ep_at * share, share).reshape(share, n_fs, head_width)
            for w in (w_query, w_key, w_value)
        ],
        axis=2,
    )
    heads_in = fs_exchange(jnp.transpose(heads_in, (1, 0, 2, 3)))
    heads_in = ep_gather(heads_in)
    w_heads = jnp.transpose(heads_in, (1, 0, 2, 3, 4)).reshape(width, 3 * head_width)

    fs_place = fs_at.reshape(1).astype(jnp.int32)
    gate_send, up_send = split_columns(fs_place, (w_gate, w_up), n_fs)
    gate_parts = fs_send(gate_send)
    up_parts = fs_send(up_send)

    expert_ids = jnp.arange(experts_total, dtype=jnp.int32)
    hit = jnp.any(routes[:, :, None] == expert_ids[None, None, :], axis=1)
    before = jnp.arange(rows_dev, dtype=jnp.int32)
    upper = (before[:, None] <= before[None, :]).astype(low_type)
    counts = mm(hit.astype(low_type), upper, TN)
    rank = jnp.where(hit.T, counts.astype(jnp.int32) - 1, -1)
    wide = jnp.concatenate([out_grad, rank.T.astype(low_type)], axis=1)
    wide = jnp.pad(wide, ((0, 0), (0, 128 - experts_total)))
    grad_all = lax.all_gather(wide, ("ep", "fs"), axis=0, tiled=True)
    base = ep_at * local_experts
    rank_all = jnp.transpose(
        grad_all[:, width : width + experts_total].reshape(devices, rows_dev, experts_total),
        (0, 2, 1),
    ).astype(jnp.int32)
    rank_rolled = jnp.roll(rank_all, -base, axis=1)
    router_rows = jnp.roll(router_full.T, -base, axis=0)

    segment, position = group_layout(
        seq_lengths[0], span_places[0], group_rows, group_rows // span_places.shape[1]
    )
    half_dim = head_dim // 2
    inverse = jnp.exp(
        jnp.arange(half_dim).astype(jnp.float32) * (-2.0 * math.log(rope_base) / head_dim)
    )
    angles = position.astype(jnp.float32)[:, None] * inverse[None, :]
    cosines = jnp.cos(angles)
    sines = jnp.sin(angles)
    cos2 = jnp.concatenate([cosines, cosines], axis=1)
    sin2 = jnp.concatenate([-sines, sines], axis=1)
    group_in = tokens_group.astype(jnp.float32)
    group_scale = rms_scale(group_in)
    normed_group = (group_in * group_scale * gain_one).astype(low_type)
    qkv = mm(normed_group, w_heads, NN)
    attended = attention_forward(qkv, gain_query, gain_key, cos2, sin2, segment, head_dim)
    branch = fs_sum(
        mm(attended, w_output, NN).astype(low_type), (*gate_parts[1:], *up_parts[1:])
    )
    hidden_in = tokens.astype(jnp.float32)
    scale_one = rms_scale(hidden_in)
    hidden_mid = hidden_in + branch
    scale_two = rms_scale(hidden_mid)
    normed_two = (hidden_mid * scale_two * gain_two).astype(low_type)

    normed_all = lax.all_gather(normed_two, ("ep", "fs"), axis=0, tiled=True)
    (out_part, dx_kept, dx_sent, dwd), dwg, dwu = run_experts(
        jnp.stack([base, fs_at, ep_at & 1]).astype(jnp.int32),
        normed_all,
        grad_all,
        rank_rolled,
        router_rows,
        gate_parts,
        up_parts,
        w_down,
        capacity,
    )
    dwg = fs_send(dwg)
    dwu = fs_send(dwu)
    dx_first = ep_halve(dx_kept, dx_sent, 0).reshape(n_ep // 2, group_rows, dx_kept.shape[1])
    dx_own = fs_sum(ep_rest(dx_first, ep_at), (*dwg[1:], *dwu[1:]))
    gate_grad = join_columns(fs_place, dwg)
    up_grad = join_columns(fs_place, dwu)

    logits = mm(normed_two, router_full, NN)
    kept = jnp.where(hit, logits, -1e30)
    powers = jnp.where(hit, jnp.exp(kept - jnp.max(kept, axis=1, keepdims=True)), 0.0)
    gates = powers / jnp.sum(powers, axis=1, keepdims=True)
    grad_gates = (
        dx_own[:, width : width + experts_total]
        + dx_own[:, width + experts_total : width + 2 * experts_total]
    )
    weighted = gates * grad_gates
    grad_logits = (weighted - gates * jnp.sum(weighted, axis=1, keepdims=True)).astype(low_type)
    router_grad = mm(normed_two, grad_logits, TN)
    grad_normed_two = dx_own[:, :width] + mm(grad_logits, router_full, NT)
    grad_mid_norm, gain_two_terms = norm_back(hidden_mid, scale_two, gain_two, grad_normed_two)
    gain_two_grad = jnp.sum(gain_two_terms, axis=0)
    grad_mid = out_grad.astype(jnp.float32) + grad_mid_norm

    branch_group = lax.all_gather(grad_mid.astype(low_type), "fs", axis=0, tiled=True)
    grad_attended = mm(branch_group, w_output, NT).astype(low_type)
    output_w_grad = mm(attended, branch_group, TN).astype(low_type)
    dq, dk, dv, dgq, dgk = attention_backward(
        qkv, grad_attended, gain_query, gain_key, cos2, sin2, segment, head_dim
    )
    grad_qkv = jnp.concatenate([dq, dk, dv], axis=1)
    heads_w_grad = mm(normed_group, grad_qkv, TN).astype(low_type)
    grad_normed_part = mm(grad_qkv, w_heads, NT)
    gain_one_grad = jnp.sum(grad_normed_part * group_in * group_scale, axis=0)
    grad_normed_one = fs_sum(grad_normed_part.astype(low_type))
    grad_in_norm, _ = norm_back(hidden_in, scale_one, gain_one, grad_normed_one)
    tokens_grad = (grad_mid + grad_in_norm).astype(low_type)

    out_w = lax.psum_scatter(output_w_grad, "ep", scatter_dimension=0, tiled=True)
    out_w = lax.ppermute(
        out_w,
        ("ep", "fs"),
        [(e * n_fs + z, z * n_ep + e) for e in range(n_ep) for z in range(n_fs)],
    ).astype(jnp.float32)
    heads_w = lax.psum_scatter(heads_w_grad, "ep", scatter_dimension=0, tiled=True)
    heads_w = fs_exchange(heads_w.reshape(n_fs, width // devices, 3 * head_width))
    heads_w = jnp.transpose(
        heads_w.reshape(n_fs, width // devices, 3, head_width), (2, 1, 0, 3)
    ).reshape(3, width // devices, width).astype(jnp.float32)

    def spread(values):
        each = head_dim // devices
        return jnp.pad(values.reshape(devices, each), ((0, 0), (0, width // devices - each))).reshape(
            width, 1
        )

    sums = jnp.concatenate(
        [
            router_grad,
            gain_two_grad[:, None],
            gain_one_grad[:, None],
            spread(jnp.sum(dgq, axis=(0, 1))),
            spread(jnp.sum(dgk, axis=(0, 1))),
        ],
        axis=1,
    )
    sums = jnp.pad(sums, ((0, 0), (0, 128 - sums.shape[1])))
    sums = fs_sum(ep_sum(sums), wire=jnp.float32)
    each = head_dim // devices

    out_group = ep_sum(out_part, (dx_own,))
    mixed = lax.psum_scatter(out_group, "fs", scatter_dimension=0, tiled=True)
    output = (hidden_mid + mixed.astype(jnp.float32)).astype(low_type)
    return (
        output,
        tokens_grad,
        sums[:, experts_total + 1],
        heads_w[0],
        heads_w[1],
        heads_w[2],
        sums[:each, experts_total + 2],
        sums[:each, experts_total + 3],
        out_w,
        sums[:, experts_total],
        sums[:, :experts_total],
        gate_grad,
        up_grad,
        dwd,
    )


def solution(mesh):
    return jax.shard_map(
        on_device,
        mesh=mesh,
        in_specs=(
            P(("ep", "fs"), None),
            P("fs"),
            P("fs", None),
            P("fs", None),
            P("fs", None),
            P("fs"),
            P("fs"),
            P("fs", None),
            P("fs"),
            P("fs", None),
            P("ep", "fs", None),
            P("ep", "fs", None),
            P("ep", "fs", None),
            P("ep", None),
            P("ep", None),
            P(("ep", "fs"), None),
            P(("ep", "fs"), None),
        ),
        out_specs=(
            P(("ep", "fs"), None),
            P(("ep", "fs"), None),
            P(("ep", "fs")),
            P(("ep", "fs"), None),
            P(("ep", "fs"), None),
            P(("ep", "fs"), None),
            P(("ep", "fs")),
            P(("ep", "fs")),
            P(("ep", "fs"), None),
            P(("ep", "fs")),
            P(("ep", "fs"), None),
            P("ep", "fs", None),
            P("ep", "fs", None),
            P("ep", "fs", None),
        ),
        check_vma=False,
    )
```
